32 devices in a mesh: dp: 8 (over y, x, core), fsdp: 4 (over z).
Axes of the slice: x: 2, y: 2, z: 4, core: 2. Of those that a mesh axis runs over, the one named last changes fastest.
Arguments:
- hidden: bfloat16 [16384, 8192], P('dp', 'fsdp'), may hold values from -50 to 50
- logit_grad: bfloat16 [16384, 256], P('dp'), may hold values from -20 to 20
- master: float32 [256, 8192], P('dp', 'fsdp'), may hold values from -6 to 6
- moment_one: float32 [256, 8192], P('dp', 'fsdp'), may hold values from -4 to 4
- moment_two: float32 [256, 8192], P('dp', 'fsdp'), may hold values from 0.25 to 4
Outputs:
- new_rows: bfloat16 [256, 8192], P(None, 'fsdp')
- new_master: float32 [256, 8192], P('dp', 'fsdp')
- new_one: float32 [256, 8192], P('dp', 'fsdp')
- new_two: float32 [256, 8192], P('dp', 'fsdp')
The draws below stay inside these ranges and needn't reach their ends.
All inputs are finite; a program needn't handle non-finite values.
Results may differ from the reference program's by a relative error of at most 0.012.
Values may be sent and summed in bfloat16 or wider, within the bound.
A program may use at most 64 MiB of HBM per device.

```python
import math
import jax
import jax.numpy as jnp
from jax import lax

D = 8192
ROW_DEV = 32
TOK_DEV = 2048
ROWS = 256
TOKENS = 16384


def token_sign(key):
    flips = jax.random.bernoulli(jax.random.fold_in(key, 41), 0.5, (TOKENS,))
    return jnp.where(flips, 1.0, -1.0).astype(jnp.float32)


def draw_hidden(key, part):
    key_col = jax.random.fold_in(key, 11)
    key_val = jax.random.fold_in(key, 12)
    key_dir = jax.random.fold_in(key, 14)
    column = jnp.arange(D, dtype=jnp.float32) / D
    colscale = 10.0 ** jax.random.uniform(key_col, (D,), jnp.float32)
    colscale = colscale * 3.0 ** column
    sign = token_sign(key)
    direction = jax.random.truncated_normal(key_dir, -2.0, 2.0, (D,), jnp.float32)
    values = jax.random.truncated_normal(key_val, -4.0, 4.0, (TOKENS, D), jnp.float32)
    amount = 0.69 * float(TOK_DEV) ** (-0.25)
    values = values + amount * sign[:, None] * direction[None, :]
    scaled = values * colscale[None, :] / 3.0
    return jnp.clip(scaled, -50.0, 50.0).astype(jnp.bfloat16)


def draw_logit_grad(key, part):
    key_row = jax.random.fold_in(key, 21)
    key_val = jax.random.fold_in(key, 22)
    key_dir = jax.random.fold_in(key, 25)
    key_cell = jax.random.fold_in(key, 26)
    blocks = TOKENS // TOK_DEV
    row_blocks = ROWS // ROW_DEV
    position = jnp.arange(ROWS, dtype=jnp.float32) / ROWS
    spread = 10.0 ** jax.random.uniform(key_row, (ROWS,), jnp.float32)
    values = jax.random.truncated_normal(key_val, -4.0, 4.0, (TOKENS, ROWS), jnp.float32)
    sign = token_sign(key)
    direction = jax.random.truncated_normal(key_dir, -2.0, 2.0, (ROWS,), jnp.float32)
    rising = 3.0 ** position
    amount = 0.69 * float(TOK_DEV) ** (-0.25)
    values = values + amount * sign[:, None] * direction[None, :]
    values = 0.006 * values * (rising * spread)[None, :]
    cell = 10.0 ** jax.random.uniform(key_cell, (blocks, row_blocks), jnp.float32, -1.0, 1.0)
    values = values.reshape(blocks, TOK_DEV, row_blocks, ROW_DEV) * cell[:, None, :, None]
    values = values.reshape(TOKENS, ROWS)
    return jnp.clip(values, -20.0, 20.0).astype(jnp.bfloat16)


def block_levels(key, extent, pieces, smallest, high):
    loudness, own = 1.0, jax.random.fold_in(key, 6)
    for dim, blocks in pieces:
        steps = jnp.exp(jax.random.uniform(jax.random.fold_in(own, dim), (blocks,), jnp.float32, smallest / len(pieces), high / len(pieces)))
        loudness = loudness * jnp.repeat(steps, extent[dim] // blocks).reshape([-1 if axis == dim else 1 for axis in range(len(extent))])
    return loudness


def noise(stream_key, dims, scale, bound, split=(), kind=jnp.bfloat16):
    values = jax.random.normal(stream_key, dims, jnp.float32) * scale
    if len(split) > 0:
        values = block_levels(stream_key, dims, split, -0.22, 0.18) * values
    return jnp.clip(values, min=-bound, max=bound).astype(kind)


def setup_inputs(seed: int = 0) -> dict:
    streams_of = jax.random.split(jax.random.key(seed), 6)
    hidden = draw_hidden(jax.random.fold_in(streams_of[5], 71), 0)
    logit_grad = draw_logit_grad(jax.random.fold_in(streams_of[5], 71), 0)
    master = noise(streams_of[2], (ROWS, D), 1.0, 6.0, ((0, 8), (1, 4)), jnp.float32)
    moment_one = noise(streams_of[3], (ROWS, D), 0.5, 4.0, ((0, 8), (1, 4)), jnp.float32)
    moment_two = jnp.clip(jnp.exp(math.log(4.0) - 2.7725887 * jax.random.uniform(streams_of[4], (ROWS, D), jnp.float32) ** block_levels(streams_of[4], (ROWS, D), ((0, 8), (1, 4)), -0.2, 0.2)), 0.25, 4.0)
    return dict(hidden=hidden, logit_grad=logit_grad, master=master, moment_one=moment_one, moment_two=moment_two)


def reference(hidden, logit_grad, master, moment_one, moment_two):
    blocks = TOKENS // TOK_DEV
    hid = hidden.reshape(blocks, TOK_DEV, D)
    lgr = logit_grad.reshape(blocks, TOK_DEV, ROWS)

    def accumulate(total, pair):
        states, grads = pair
        part = lax.dot_general(grads, states, (((0,), (0,)), ((), ())), preferred_element_type=jnp.float32)
        part = lax.optimization_barrier(part.astype(jnp.bfloat16)).astype(jnp.float32)
        return (total + part, None)
    grad, _ = lax.scan(accumulate, jnp.zeros((ROWS, D), jnp.float32), (hid, lgr))
    sumsq = jnp.sum(grad * grad)
    rms = jnp.sqrt(sumsq / (ROWS * D))
    factor = jnp.minimum(1.0, 1.0 / rms)
    clipped = factor * grad
    new_one = 0.9 * moment_one + 0.1 * clipped
    new_two = 0.95 * moment_two + 0.05 * clipped * clipped
    first = new_one / (1.0 - 0.9 ** 10)
    second = new_two / (1.0 - 0.95 ** 10)
    new_master = master - 0.05 * (first / (jnp.sqrt(second) + 1e-08) + 0.1 * master)
    return (new_master.astype(jnp.bfloat16), new_master, new_one, new_two)
```

```python
import functools

import jax
import jax.numpy as jnp
from jax import lax
from jax.experimental import pallas as pl
from jax.experimental.pallas import tpu as pltpu
from jax.sharding import PartitionSpec as P

MESH = pl.DeviceIdType.MESH
LOAD_CHUNKS = 4
GATHER_CHUNKS = 2


def pieces(width, wanted):
    count = wanted
    while count > 1 and width % (count * 128):
        count -= 1
    return count


def kernel(
    n, depth, chunks, gathers,
    hid, lgr, mas, one, two,
    rows_out, mas_out, one_out, two_out,
    lgr_v, lgt_v, hid_v, mas_v, one_v, two_v,
    stage, paired, sums, arrived, grad, sq_all, gath,
    hid_sem, lgr_sem, state_sem, pair_send, pair_recv, chip_send, chip_recv,
    sq_send, sq_recv, ag_send, ag_recv, relay_send, relay_recv, rows_sem, out_sem,
):
    chips = n // 2
    total = n * depth
    rows, width = grad.shape
    dp, fs = lax.axis_index("dp"), lax.axis_index("fsdp")
    chip, core = dp // 2, dp % 2
    other = 1 - core
    me = dp * depth + fs
    wc, wa = width // chunks, width // gathers

    lgr_copy = pltpu.make_async_copy(lgr, lgr_v, lgr_sem)
    lgr_copy.start()
    loads = []
    for j in range(chunks):
        load = pltpu.make_async_copy(hid.at[:, pl.ds(j * wc, wc)], hid_v.at[j], hid_sem.at[j])
        load.start()
        loads.append(load)
    states = []
    for i, (src, dst) in enumerate(((mas, mas_v), (one, one_v), (two, two_v))):
        load = pltpu.make_async_copy(src, dst, state_sem.at[i])
        load.start()
        states.append(load)

    def each_other_device(act):
        def visit(i):
            index = (me + i) % total
            act((index // depth, index % depth))

        if total <= 64:
            for i in range(1, total):
                visit(i)
        else:
            lax.fori_loop(1, total, lambda i, carry: (visit(i), carry)[1], 0)

    barrier = pltpu.get_barrier_semaphore()
    each_other_device(
        lambda to: pl.semaphore_signal(barrier, inc=1, device_id=to, device_id_type=MESH)
    )

    lgr_copy.wait()
    lgt_v[...] = lgr_v[...].T

    def remote(src, dst, send, recv, to):
        return pltpu.make_async_remote_copy(
            src_ref=src, dst_ref=dst, send_sem=send, recv_sem=recv, device_id=to, device_id_type=MESH
        )

    partner = (2 * chip + other, fs)
    others = [(chip + o) % chips for o in range(1, chips)]

    def pair_copy(j):
        return remote(stage.at[j, other], paired.at[j], pair_send.at[j], pair_recv.at[j], partner)

    def chip_copy(j, q, slot):
        return remote(
            sums.at[j, q], arrived.at[j, slot], chip_send.at[j, q], chip_recv.at[j, slot],
            (2 * q + core, fs),
        )

    def chip_sum(j):
        pair_copy(j).wait_recv()
        for q in others:
            both = stage[j, core, q].astype(jnp.float32) + paired[j, q].astype(jnp.float32)
            sums[j, q] = both.astype(jnp.bfloat16)
            chip_copy(j, q, chip).start()
        grad[:, pl.ds(j * wc, wc)] = stage[j, core, chip].astype(jnp.float32) + paired[
            j, chip
        ].astype(jnp.float32)

    for j in range(chunks):
        loads[j].wait()
        part = jnp.dot(lgt_v[...], hid_v[j], preferred_element_type=jnp.float32)
        part = part.astype(jnp.bfloat16)
        for q in range(chips):
            for c in range(2):
                d = 2 * q + c
                stage[j, c, q] = part[d * rows : (d + 1) * rows, :]
        if j == 0:
            pl.semaphore_wait(barrier, total - 1)
        pair_copy(j).start()
        if j > 0:
            chip_sum(j - 1)
    chip_sum(chunks - 1)

    squares = jnp.zeros((1, 128), jnp.float32)
    for j in range(chunks):
        span = pl.ds(j * wc, wc)
        value = grad[:, span]
        for q in others:
            chip_copy(j, q, q).wait_recv()
            value = value + arrived[j, q].astype(jnp.float32)
        grad[:, span] = value
        column = jnp.sum(value * value, axis=0, keepdims=True)
        for s in range(wc // 128):
            squares = squares + column[:, s * 128 : (s + 1) * 128]

    sq_all[me] = squares
    each_other_device(
        lambda to: remote(sq_all.at[me], sq_all.at[me], sq_send, sq_recv, to).start()
    )
    for load in states:
        load.wait()
    everyone = sq_all.at[pl.ds(0, total - 1)]
    pltpu.make_async_copy(everyone, everyone, sq_recv).wait()
    sumsq = jnp.sum(jnp.sum(sq_all[...], axis=0), axis=1, keepdims=True)
    rms = jnp.sqrt(sumsq / (rows * n * width * depth))
    factor = jnp.where(rms > 1.0, 1.0 / rms, 1.0)

    def cols(k):
        return pl.ds(k * wa, wa)

    def gather_copy(k, d, to, send, recv):
        block = gath.at[d, :, cols(k)]
        return remote(block, block, send, recv, to)

    def direct(k, source, q):
        return gather_copy(k, 2 * source + core, (2 * q + core, fs), ag_send.at[k, q], ag_recv.at[k, source])

    def relay(k, q, side):
        return gather_copy(k, 2 * q + side, partner, relay_send.at[k, q], relay_recv.at[k, q])

    def put_rows(k, d):
        pltpu.make_async_copy(
            gath.at[d, :, cols(k)],
            rows_out.at[pl.ds(pl.multiple_of(d * rows, rows), rows), cols(k)],
            rows_sem,
        ).start()

    for k in range(gathers):
        span = cols(k)
        clipped = factor * grad[:, span]
        new_one = 0.9 * one_v[:, span] + 0.1 * clipped
        new_two = 0.95 * two_v[:, span] + 0.05 * clipped * clipped
        first = new_one / (1.0 - 0.9**10)
        second = new_two / (1.0 - 0.95**10)
        held = mas_v[:, span]
        new_master = held - 0.05 * (first / (jnp.sqrt(second) + 1e-08) + 0.1 * held)
        gath[dp, :, span] = new_master.astype(jnp.bfloat16)
        for q in others:
            direct(k, chip, q).start()
        relay(k, chip, core).start()
        put_rows(k, dp)
        one_v[:, span] = new_one
        two_v[:, span] = new_two
        mas_v[:, span] = new_master
    outs = []
    for i, (src, dst) in enumerate(((mas_v, mas_out), (one_v, one_out), (two_v, two_out))):
        out = pltpu.make_async_copy(src, dst, out_sem.at[i])
        out.start()
        outs.append(out)
    for k in range(gathers):
        for q in others:
            direct(k, q, q).wait_recv()
            relay(k, q, core).start()
            put_rows(k, 2 * q + core)
    for k in range(gathers):
        for q in [chip] + others:
            relay(k, q, other).wait_recv()
            put_rows(k, 2 * q + other)

    for j in range(chunks):
        pair_copy(j).wait_send()
        for q in others:
            chip_copy(j, q, chip).wait_send()
    pltpu.make_async_copy(everyone, everyone, sq_send).wait()
    for k in range(gathers):
        for q in others:
            direct(k, chip, q).wait_send()
            relay(k, q, core).wait_send()
        relay(k, chip, core).wait_send()
    for out in outs:
        out.wait()
    pltpu.make_async_copy(rows_out, rows_out, rows_sem).wait()


def shards(n, depth, hidden, logit_grad, master, moment_one, moment_two):
    tokens, width = hidden.shape
    slab = logit_grad.shape[1]
    rows = master.shape[0]
    chips = n // 2
    chunks = pieces(width, LOAD_CHUNKS)
    gathers = pieces(width, GATHER_CHUNKS)
    wc = width // chunks
    f32, bf16 = jnp.float32, jnp.bfloat16
    state = jax.ShapeDtypeStruct((rows, width), f32)
    dma = pltpu.SemaphoreType.DMA
    anywhere = pl.BlockSpec(memory_space=pl.ANY)
    return pl.pallas_call(
        functools.partial(kernel, n, depth, chunks, gathers),
        out_shape=(jax.ShapeDtypeStruct((slab, width), bf16), state, state, state),
        in_specs=[anywhere] * 5,
        out_specs=(anywhere,) * 4,
        scratch_shapes=[
            pltpu.VMEM((tokens, slab), bf16),
            pltpu.VMEM((slab, tokens), bf16),
            pltpu.VMEM((chunks, tokens, wc), bf16),
            pltpu.VMEM((rows, width), f32),
            pltpu.VMEM((rows, width), f32),
            pltpu.VMEM((rows, width), f32),
            pltpu.VMEM((chunks, 2, chips, rows, wc), bf16),
            pltpu.VMEM((chunks, chips, rows, wc), bf16),
            pltpu.VMEM((chunks, chips, rows, wc), bf16),
            pltpu.VMEM((chunks, chips, rows, wc), bf16),
            pltpu.VMEM((rows, width), f32),
            pltpu.VMEM((n * depth, 1, 128), f32),
            pltpu.VMEM((n, rows, width), bf16),
            dma((chunks,)),
            dma,
            dma((3,)),
            dma((chunks,)),
            dma((chunks,)),
            dma((chunks, chips)),
            dma((chunks, chips)),
            dma,
            dma,
            dma((gathers, chips)),
            dma((gathers, chips)),
            dma((gathers, chips)),
            dma((gathers, chips)),
            dma,
            dma((3,)),
        ],
        compiler_params=pltpu.CompilerParams(
            collective_id=0, has_side_effects=True, vmem_limit_bytes=60 * 1024 * 1024
        ),
    )(hidden, logit_grad, master, moment_one, moment_two)


def solution(mesh):
    placed = (P("dp", "fsdp"), P("dp", None), P("dp", "fsdp"), P("dp", "fsdp"), P("dp", "fsdp"))
    return jax.shard_map(
        functools.partial(shards, mesh.shape["dp"], mesh.shape["fsdp"]),
        mesh=mesh,
        in_specs=placed,
        out_specs=(P(None, "fsdp"), P("dp", "fsdp"), P("dp", "fsdp"), P("dp", "fsdp")),
        check_vma=False,
    )
```

```python
import functools

import jax
import jax.numpy as jnp
from jax import lax
from jax.experimental import pallas as pl
from jax.experimental.pallas import tpu as pltpu
from jax.sharding import PartitionSpec as P

MESH = pl.DeviceIdType.MESH
LOAD_CHUNKS = 4
GATHER_CHUNKS = 2
VMEM_BYTES = 67_043_328


def pieces(width, wanted):
    count = wanted
    while count > 1 and width % (count * 128):
        count -= 1
    return count


def kernel(
    n, depth, chunks, gathers,
    hid, lgr, mas, one, two,
    rows_out, mas_out, one_out, two_out,
    lgr_v, lgt_v, hid_v, mas_v, one_v, two_v,
    stage, paired, sums, arrived, grad, sq_all,
    hid_sem, lgr_sem, state_sem, pair_send, pair_recv, chip_send, chip_recv,
    sq_send, sq_recv, ag_send, ag_recv, relay_send, relay_recv,
):
    chips = n // 2
    total = n * depth
    rows, width = grad.shape
    dp, fs = lax.axis_index("dp"), lax.axis_index("fsdp")
    chip, core = dp // 2, dp % 2
    other = 1 - core
    me = dp * depth + fs
    wc, wa = width // chunks, width // gathers

    lgr_copy = pltpu.make_async_copy(lgr, lgr_v, lgr_sem)
    lgr_copy.start()
    loads = []
    for j in range(chunks):
        load = pltpu.make_async_copy(hid.at[:, pl.ds(j * wc, wc)], hid_v.at[j], hid_sem.at[j])
        load.start()
        loads.append(load)
    states = []
    for i, (src, dst) in enumerate(((mas, mas_v), (one, one_v), (two, two_v))):
        load = pltpu.make_async_copy(src, dst, state_sem.at[i])
        load.start()
        states.append(load)

    def each_other_device(act):
        def visit(i):
            index = (me + i) % total
            act((index // depth, index % depth))

        if total <= 64:
            for i in range(1, total):
                visit(i)
        else:
            lax.fori_loop(1, total, lambda i, carry: (visit(i), carry)[1], 0)

    barrier = pltpu.get_barrier_semaphore()
    each_other_device(
        lambda to: pl.semaphore_signal(barrier, inc=1, device_id=to, device_id_type=MESH)
    )

    lgr_copy.wait()
    lgt_v[...] = lgr_v[...].T

    def remote(src, dst, send, recv, to):
        return pltpu.make_async_remote_copy(
            src_ref=src, dst_ref=dst, send_sem=send, recv_sem=recv, device_id=to, device_id_type=MESH
        )

    partner = (2 * chip + other, fs)
    others = [(chip + o) % chips for o in range(1, chips)]

    def pair_copy(j):
        return remote(stage.at[j, other], paired.at[j], pair_send.at[j], pair_recv.at[j], partner)

    def chip_copy(j, q, slot):
        return remote(
            sums.at[j, q], arrived.at[j, slot], chip_send.at[j, q], chip_recv.at[j, slot],
            (2 * q + core, fs),
        )

    def chip_sum(j):
        pair_copy(j).wait_recv()
        for q in others:
            both = stage[j, core, q].astype(jnp.float32) + paired[j, q].astype(jnp.float32)
            sums[j, q] = both.astype(jnp.bfloat16)
            chip_copy(j, q, chip).start()
        grad[:, pl.ds(j * wc, wc)] = stage[j, core, chip].astype(jnp.float32) + paired[
            j, chip
        ].astype(jnp.float32)

    for j in range(chunks):
        loads[j].wait()
        part = jnp.dot(lgt_v[...], hid_v[j], preferred_element_type=jnp.float32)
        part = part.astype(jnp.bfloat16)
        for q in range(chips):
            for c in range(2):
                d = 2 * q + c
                stage[j, c, q] = part[d * rows : (d + 1) * rows, :]
        if j == 0:
            pl.semaphore_wait(barrier, total - 1)
        pair_copy(j).start()
        if j > 0:
            chip_sum(j - 1)
    chip_sum(chunks - 1)

    squares = jnp.zeros((1, 128), jnp.float32)
    for j in range(chunks):
        span = pl.ds(j * wc, wc)
        value = grad[:, span]
        for q in others:
            chip_copy(j, q, q).wait_recv()
            value = value + arrived[j, q].astype(jnp.float32)
        grad[:, span] = value
        column = jnp.sum(value * value, axis=0, keepdims=True)
        for s in range(wc // 128):
            squares = squares + column[:, s * 128 : (s + 1) * 128]

    sq_all[me] = squares
    each_other_device(
        lambda to: remote(sq_all.at[me], sq_all.at[me], sq_send, sq_recv, to).start()
    )
    for load in states:
        load.wait()
    everyone = sq_all.at[pl.ds(0, total - 1)]
    pltpu.make_async_copy(everyone, everyone, sq_recv).wait()
    sumsq = jnp.sum(jnp.sum(sq_all[...], axis=0), axis=1, keepdims=True)
    rms = jnp.sqrt(sumsq / (rows * n * width * depth))
    factor = jnp.where(rms > 1.0, 1.0 / rms, 1.0)

    def cols(k):
        return pl.ds(k * wa, wa)

    def rows_of(d):
        return pl.ds(pl.multiple_of(d * rows, rows), rows)

    def gather_copy(k, d, to, send, recv):
        block = rows_out.at[rows_of(d), cols(k)]
        return remote(block, block, send, recv, to)

    def direct(k, source, q):
        return gather_copy(k, 2 * source + core, (2 * q + core, fs), ag_send.at[k, q], ag_recv.at[k, source])

    def relay(k, q, side):
        return gather_copy(k, 2 * q + side, partner, relay_send.at[k, q], relay_recv.at[k, q])

    for k in range(gathers):
        span = cols(k)
        clipped = factor * grad[:, span]
        new_one = 0.9 * one_v[:, span] + 0.1 * clipped
        new_two = 0.95 * two_v[:, span] + 0.05 * clipped * clipped
        first = new_one / (1.0 - 0.9**10)
        second = new_two / (1.0 - 0.95**10)
        held = mas_v[:, span]
        new_master = held - 0.05 * (first / (jnp.sqrt(second) + 1e-08) + 0.1 * held)
        rows_out[rows_of(dp), span] = new_master.astype(jnp.bfloat16)
        for q in others:
            direct(k, chip, q).start()
        relay(k, chip, core).start()
        one_out[:, span] = new_one
        two_out[:, span] = new_two
        mas_out[:, span] = new_master
    for k in range(gathers):
        for q in others:
            direct(k, q, q).wait_recv()
            relay(k, q, core).start()
    for k in range(gathers):
        for q in [chip] + others:
            relay(k, q, other).wait_recv()

    for j in range(chunks):
        pair_copy(j).wait_send()
        for q in others:
            chip_copy(j, q, chip).wait_send()
    pltpu.make_async_copy(everyone, everyone, sq_send).wait()
    for k in range(gathers):
        for q in others:
            direct(k, chip, q).wait_send()
            relay(k, q, core).wait_send()
        relay(k, chip, core).wait_send()


def write_out(*refs):
    sems = refs[8]
    copies = [pltpu.make_async_copy(refs[i], refs[4 + i], sems.at[i]) for i in range(4)]
    for copy in copies:
        copy.start()
    for copy in copies:
        copy.wait()


def shards(n, depth, hidden, logit_grad, master, moment_one, moment_two):
    tokens, width = hidden.shape
    slab = logit_grad.shape[1]
    rows = master.shape[0]
    chips = n // 2
    chunks = pieces(width, LOAD_CHUNKS)
    gathers = pieces(width, GATHER_CHUNKS)
    wc = width // chunks
    f32, bf16 = jnp.float32, jnp.bfloat16
    state = ((rows, width), f32)
    shapes = (((slab, width), bf16), state, state, state)
    kept = slab * width * 2 + 3 * rows * width * 4
    dma = pltpu.SemaphoreType.DMA
    anywhere = pl.BlockSpec(memory_space=pl.ANY)
    in_vmem = pl.BlockSpec(memory_space=pltpu.VMEM)
    held = pl.pallas_call(
        functools.partial(kernel, n, depth, chunks, gathers),
        out_shape=tuple(pltpu.VMEM(*shape) for shape in shapes),
        in_specs=[anywhere] * 5,
        out_specs=(in_vmem,) * 4,
        scratch_shapes=[
            pltpu.VMEM((tokens, slab), bf16),
            pltpu.VMEM((slab, tokens), bf16),
            pltpu.VMEM((chunks, tokens, wc), bf16),
            pltpu.VMEM((rows, width), f32),
            pltpu.VMEM((rows, width), f32),
            pltpu.VMEM((rows, width), f32),
            pltpu.VMEM((chunks, 2, chips, rows, wc), bf16),
            pltpu.VMEM((chunks, chips, rows, wc), bf16),
            pltpu.VMEM((chunks, chips, rows, wc), bf16),
            pltpu.VMEM((chunks, chips, rows, wc), bf16),
            pltpu.VMEM((rows, width), f32),
            pltpu.VMEM((n * depth, 1, 128), f32),
            dma((chunks,)),
            dma,
            dma((3,)),
            dma((chunks,)),
            dma((chunks,)),
            dma((chunks, chips)),
            dma((chunks, chips)),
            dma,
            dma,
            dma((gathers, chips)),
            dma((gathers, chips)),
            dma((gathers, chips)),
            dma((gathers, chips)),
        ],
        compiler_params=pltpu.CompilerParams(
            collective_id=0, has_side_effects=True, vmem_limit_bytes=VMEM_BYTES - kept - 96 * 1024
        ),
    )(hidden, logit_grad, master, moment_one, moment_two)
    return pl.pallas_call(
        write_out,
        out_shape=tuple(pltpu.HBM(*shape) for shape in shapes),
        in_specs=[anywhere] * 4,
        out_specs=(anywhere,) * 4,
        scratch_shapes=[dma((4,))],
        compiler_params=pltpu.CompilerParams(vmem_limit_bytes=1024 * 1024),
    )(*held)


def solution(mesh):
    placed = (P("dp", "fsdp"), P("dp", None), P("dp", "fsdp"), P("dp", "fsdp"), P("dp", "fsdp"))
    return jax.shard_map(
        functools.partial(shards, mesh.shape["dp"], mesh.shape["fsdp"]),
        mesh=mesh,
        in_specs=placed,
        out_specs=(P(None, "fsdp"), P("dp", "fsdp"), P("dp", "fsdp"), P("dp", "fsdp")),
        check_vma=False,
    )
```
